256 devices in a mesh: rep: 1, dp: 256 (over x, y, z, core).
Axes of the slice: x: 4, y: 4, z: 8, core: 2. Of those that a mesh axis runs over, the one named last changes fastest.
Arguments:
- x: bfloat16 [256, 1024, 768], P(('rep', 'dp'))
- dy: bfloat16 [256, 1024, 768], P(('rep', 'dp'))
- wq: bfloat16 [1, 768, 1024], replicated
- wk: bfloat16 [1, 768, 1024], replicated
- wv: bfloat16 [1, 768, 1024], replicated
- wo: bfloat16 [1, 1024, 768], replicated
- w_gate: bfloat16 [1, 768, 6144], replicated
- w_up: bfloat16 [1, 768, 6144], replicated
- w_down: bfloat16 [1, 6144, 768], replicated
- m_wq: float32 [1, 768, 1024], replicated
- m_wk: float32 [1, 768, 1024], replicated
- m_wv: float32 [1, 768, 1024], replicated
- m_wo: float32 [1, 1024, 768], replicated
- m_w_gate: float32 [1, 768, 6144], replicated
- m_w_up: float32 [1, 768, 6144], replicated
- m_w_down: float32 [1, 6144, 768], replicated
- v_wq: float32 [1, 768, 1024], replicated
- v_wk: float32 [1, 768, 1024], replicated
- v_wv: float32 [1, 768, 1024], replicated
- v_wo: float32 [1, 1024, 768], replicated
- v_w_gate: float32 [1, 768, 6144], replicated
- v_w_up: float32 [1, 768, 6144], replicated
- v_w_down: float32 [1, 6144, 768], replicated
Outputs:
- output 1: bfloat16 [1, 768, 1024], P('rep')
- output 2: bfloat16 [1, 768, 1024], P('rep')
- output 3: bfloat16 [1, 768, 1024], P('rep')
- output 4: bfloat16 [1, 1024, 768], P('rep')
- output 5: bfloat16 [1, 768, 6144], P('rep')
- output 6: bfloat16 [1, 768, 6144], P('rep')
- output 7: bfloat16 [1, 6144, 768], P('rep')
- output 8: float32 [1, 768, 1024], P('rep')
- output 9: float32 [1, 768, 1024], P('rep')
- output 10: float32 [1, 768, 1024], P('rep')
- output 11: float32 [1, 1024, 768], P('rep')
- output 12: float32 [1, 768, 6144], P('rep')
- output 13: float32 [1, 768, 6144], P('rep')
- output 14: float32 [1, 6144, 768], P('rep')
- output 15: float32 [1, 768, 1024], P('rep')
- output 16: float32 [1, 768, 1024], P('rep')
- output 17: float32 [1, 768, 1024], P('rep')
- output 18: float32 [1, 1024, 768], P('rep')
- output 19: float32 [1, 768, 6144], P('rep')
- output 20: float32 [1, 768, 6144], P('rep')
- output 21: float32 [1, 6144, 768], P('rep')
All inputs are finite; a program needn't handle non-finite values.
Results may differ from the reference program's by a relative error of at most 0.024.
Values are sent between devices in bfloat16 or wider.
A program may use at most 768 MiB of HBM per device.

```python
import jax
import jax.numpy as jnp
from jax import lax

SEQUENCES = 256
TOKENS = 1024
D = 768
HEADS = 4
KV_HEADS = 4
HEAD = 256
FF = 6144
LAYERS = 1
THETA = 10000
NAMES = ("wq", "wk", "wv", "wo", "w_gate", "w_up", "w_down")
SHAPES = {
    "wq": (LAYERS, D, HEADS * HEAD),
    "wk": (LAYERS, D, KV_HEADS * HEAD),
    "wv": (LAYERS, D, KV_HEADS * HEAD),
    "wo": (LAYERS, HEADS * HEAD, D),
    "w_gate": (LAYERS, D, FF),
    "w_up": (LAYERS, D, FF),
    "w_down": (LAYERS, FF, D),
}


def bump(key, n, height):
    away = (jnp.arange(n, dtype=jnp.int32) - jax.random.randint(key, (), 0, n, jnp.int32)) % n
    return jnp.where(away < n // 8, height, 1.0)


def together(key, own, strength):
    shared = jax.random.normal(key, own.shape[1:], jnp.float32)
    return (own + strength * shared) * lax.rsqrt(1 + strength * strength)


def setup_inputs(seed: int = 0, part: int = 0) -> dict:
    kx, kdy, ka, kb, kz, kf, kh, kl, *keys = jax.random.split(jax.random.key(seed), 8 + 3 * len(NAMES))
    kx, kdy, ka, kb = (jax.random.fold_in(k, part) for k in (kx, kdy, ka, kb))
    kw, km, kv = (keys[i::3] for i in range(3))
    shape = (SEQUENCES, TOKENS, D)
    much_x, much_dy = jax.random.uniform(kz, (2,), jnp.float32, 0.0, 1.0)
    loud = 2.0 ** jax.random.uniform(jax.random.fold_in(kz, 1), (), jnp.float32, -1.0, 2.0)
    layers = 2.0 ** jax.random.uniform(kl, (LAYERS, 1, 1), jnp.float32, -1.0, 1.0)
    times = {"wq": 1.0, "wk": 1.0, "wv": 2.0, "wo": layers, "w_gate": 1.0, "w_up": bump(kh, FF, 4.0), "w_down": layers}
    x = together(ka, jax.random.normal(kx, shape, jnp.float32), much_x) * bump(kf, D, 4.0)
    dy = together(kb, jax.random.normal(kdy, shape, jnp.float32), much_dy)
    drawn = {"x": x.astype(jnp.bfloat16), "dy": (loud * dy * (SEQUENCES * TOKENS) ** -0.5).astype(jnp.bfloat16)}
    for key, name in zip(kw, NAMES, strict=True):
        drawn[name] = (jax.random.normal(key, SHAPES[name], jnp.float32) * SHAPES[name][1] ** -0.5 * times[name]).astype(jnp.bfloat16)
    for key, name in zip(km, NAMES, strict=True):
        drawn[f"m_{name}"] = 0.1 * jax.random.normal(key, SHAPES[name], jnp.float32)
    for key, name in zip(kv, NAMES, strict=True):
        drawn[f"v_{name}"] = jax.random.uniform(key, SHAPES[name], jnp.float32, 0.02, 0.06)
    return drawn


def matmul(a, w):
    return jnp.dot(a, w, preferred_element_type=jnp.float32).astype(jnp.bfloat16)


def normed(h):
    wide = h.astype(jnp.float32)
    scale = lax.rsqrt(jnp.mean(wide**2, -1, keepdims=True) + 1e-6)
    return (wide * scale).astype(jnp.bfloat16)


def turned(t, theta):
    half = t.shape[-1] // 2
    angle = jnp.arange(t.shape[0], dtype=jnp.float32)[:, None] * theta ** (-jnp.arange(half, dtype=jnp.float32) / half)
    cos, sin = jnp.cos(angle)[:, None], jnp.sin(angle)[:, None]
    a, b = t[..., :half].astype(jnp.float32), t[..., half:].astype(jnp.float32)
    return jnp.concatenate([a * cos - b * sin, b * cos + a * sin], -1).astype(jnp.bfloat16)


def seen_by(q, k, v):
    tokens, kv = q.shape[0], k.shape[1]
    q = q.reshape(tokens, kv, -1, q.shape[-1])
    scores = jnp.einsum("tgsd,ugd->gstu", q.astype(jnp.float32), k.astype(jnp.float32)) * q.shape[-1] ** -0.5
    place = jnp.arange(tokens)
    weights = jax.nn.softmax(jnp.where(place[:, None] >= place, scores, -jnp.inf), -1).astype(jnp.bfloat16)
    return jnp.einsum("gstu,ugd->tgsd", weights.astype(jnp.float32), v.astype(jnp.float32)).astype(jnp.bfloat16).reshape(tokens, -1)


def layer(h, w):
    a = normed(h)
    q, k = (turned(matmul(a, w[name]).reshape(h.shape[0], -1, HEAD), THETA) for name in ("wq", "wk"))
    h = h + matmul(seen_by(q, k, matmul(a, w["wv"]).reshape(h.shape[0], -1, HEAD)), w["wo"])
    b = normed(h)
    gate = jnp.dot(b, w["w_gate"], preferred_element_type=jnp.float32)
    up = jnp.dot(b, w["w_up"], preferred_element_type=jnp.float32)
    return h + matmul((jax.nn.silu(gate) * up).astype(jnp.bfloat16), w["w_down"])


def adamw(w, m, v, g):
    m = 0.9 * m + 0.1 * g
    v = 0.95 * v + 0.05 * g * g
    step = m * lax.rsqrt(v + 1e-8) + 0.1 * w
    return (w - 0.02 * step).astype(jnp.bfloat16), m, v


def clipped(gradients, sum_of_squares, count):
    factor = jnp.minimum(1.0, 0.5 * lax.rsqrt(sum_of_squares / count + 1e-30))
    return [g * factor for g in gradients]


def stack(weights, h):
    return lax.scan(lambda h, w: (layer(h, w), None), h, weights)[0]


def reference(x, dy, wq, wk, wv, wo, w_gate, w_up, w_down, m_wq, m_wk, m_wv, m_wo, m_w_gate, m_w_up, m_w_down, v_wq, v_wk, v_wv, v_wo, v_w_gate, v_w_up, v_w_down):
    weights = dict(zip(NAMES, (wq, wk, wv, wo, w_gate, w_up, w_down), strict=True))

    def take(so_far, sequence):
        h, by_y = sequence
        _, back = jax.vjp(stack, weights, h)
        by_weights, by_h = back(by_y)
        return jax.tree.map(lambda total, term: total + term.astype(jnp.float32), so_far, by_weights), by_h

    none_yet = {name: jnp.zeros(w.shape, jnp.float32) for name, w in weights.items()}
    by_weights, by_x = lax.scan(take, none_yet, (x, dy))
    gradients = [by_weights[name].astype(jnp.bfloat16).astype(jnp.float32) for name in NAMES]
    gradients = clipped(gradients, sum(jnp.sum(g * g) for g in gradients), sum(g.size for g in gradients))
    first = (m_wq, m_wk, m_wv, m_wo, m_w_gate, m_w_up, m_w_down)
    second = (v_wq, v_wk, v_wv, v_wo, v_w_gate, v_w_up, v_w_down)
    new = [adamw(weights[name].astype(jnp.float32), m, v, g) for name, m, v, g in zip(NAMES, first, second, gradients, strict=True)]
    return tuple(one[which] for which in range(3) for one in new)
```

```python
import functools

import jax
import jax.numpy as jnp
from jax import lax
from jax.experimental import pallas as pl
from jax.experimental.pallas import tpu as pltpu
from jax.sharding import PartitionSpec as P

MESH = pl.DeviceIdType.MESH
F32, BF16 = jnp.float32, jnp.bfloat16
VMEM = 61 * 2**20
HEAD = 256
THETA = 10000
LOG2E = 1.4426950408889634
SCALE = HEAD**-0.5
HIDDEN = -1e30
WIDE = 512
TILE = (8, 128)
ZS = range(1, 8)
BOTH = range(2)
STEP = 48
BLOCK = 512
CHUNKS = 12
HEADS = 4
QUERIES = 256


def _dot(a, b):
    return jnp.dot(a, b, preferred_element_type=F32)


def _dot_t(a, b):
    return lax.dot_general(a, b, (((1,), (1,)), ((), ())), preferred_element_type=F32)


def _down(reduce, x):
    return reduce(x, 0, keepdims=True)


def _mean(x):
    return jnp.mean(x, -1, keepdims=True)


def _origin(shape):
    return lambda _: (0,) * len(shape)


def mix(bit, if0, if1):
    return if0 * (1 - bit) + if1 * bit


class Geo:
    def __init__(self, rows, per_group):
        self.rows, self.nq = rows, per_group
        self.h0, self.hp, self.h1, self.h2 = rows // 2, rows // 4, rows // 8, rows // 16
        self.pieces = 4 // per_group
        self.pr = self.h2 // self.pieces
        self.kept = (self.h1, 512), (self.h2, 512), (self.h2, 256), (self.h2, 128)


FFN, ATT = Geo(2304, 4), Geo(3072, 2)
GROUPS = CHUNKS // FFN.nq


class Place:
    def __init__(self):
        d = lax.axis_index("dp")
        core, z, y, x = d % 2, (d // 2) % 8, (d // 16) % 4, d // 64
        self.core, self.z = core, z
        at = lambda x, y, z, core: ((x * 4 + y) * 8 + z) * 2 + core
        other = lambda c, kind: c + 1 - 2 * (c % 2) if kind == 1 else 3 - c
        half = lambda c, kind: ((c + 1) // 2) % 2 if kind == 1 else c // 2
        swap = {("x", k): (at(other(x, k), y, z, core), half(x, k)) for k in (1, 3)}
        swap.update({("y", k): (at(x, other(y, k), z, core), half(y, k)) for k in (1, 3)})
        order = ("x", 1), ("x", 3), ("y", 1), ("y", 3)
        self.fixed = [swap[key][0] for key in order]
        both = [[(swap[a, k], swap[a, 4 - k]) for a, k in keys] for keys in (order, order[::-1])]
        self.peer = [[mix(core, one[0], two[0]) for one, two in part] for part in both]
        self.bit = [[mix(core, one[1], two[1]) for one, two in part] for part in both]
        self.partner = at(x, y, z, 1 - core)
        self.zpeer = lambda k: at(x, y, (z + k) % 8, core)
        self.all_peers = [self.partner, *self.fixed, *(self.zpeer(k) for k in ZS)]

    def where(self, geo, p, swaps):
        b = self.bit[p] if isinstance(p, int) else [mix(p, *pair) for pair in zip(*self.bit, strict=True)]
        row = self.core * geo.h0 + p * geo.hp + b[0] * geo.h1
        return row + b[1] * geo.h2 if swaps > 1 else row, b[2] * 256, b[2] * 256 + b[3] * 128


def rep_index():
    return lax.axis_index("rep")


def to(src, dst, send, recv, device):
    return pltpu.make_async_remote_copy(src_ref=src, dst_ref=dst, send_sem=send, recv_sem=recv, device_id=(rep_index(), device),
                                        device_id_type=MESH)


def greet(place):
    barrier = pltpu.get_barrier_semaphore()
    for peer in place.all_peers:
        pl.semaphore_signal(barrier, inc=1, device_id=(rep_index(), peer), device_id_type=MESH)


def greeted(place):
    pl.semaphore_wait(pltpu.get_barrier_semaphore(), len(place.all_peers))


def rows_of(start, size):
    return pl.ds(pl.multiple_of(start, 16), size)


def cols_of(start, size):
    return pl.ds(pl.multiple_of(start, 128), size)


def strips(rows, body):
    lax.fori_loop(0, rows // STEP, lambda i, _: body(pl.multiple_of(i * STEP, STEP)), None)


def rs_scratch():
    v, dma = pltpu.VMEM, pltpu.SemaphoreType.DMA
    out = [v((2, ATT.h0, WIDE), BF16), dma((1,)), dma((2,)), dma((4, 2)), dma((4, 2, 2))]
    for kept in ATT.kept:
        out += [v((2, *kept), BF16), v((2, *kept), F32), v((2, 2, *kept), BF16)]
    for geo, groups in ((FFN, GROUPS), (ATT, 1)):
        out += [v((8, geo.pr, 128), BF16), v((8, geo.pr, 128), F32), v((groups, 8, geo.pr, 128), BF16), dma((8,)), dma((groups, 8))]
    return out


class ReduceScatter:
    def __init__(self, place, refs):
        self.place = place
        self.l0, self.d_send, self.d_recv, self.s_send, self.s_recv = refs[:5]
        swaps, items = refs[5:17], refs[17:]
        self.s, self.k, self.l = swaps[0::3], swaps[1::3], swaps[2::3]
        self.items = {FFN: items[:5], ATT: items[5:]}

    def swap0(self, geo, own, slot):
        return to(own.at[rows_of((1 - self.place.core) * geo.h0, geo.h0), :], self.l0.at[slot, pl.ds(0, geo.h0), :], self.d_send.at[0],
                  self.d_recv.at[slot], self.place.partner)

    def swap(self, geo, stage, part, slot):
        rows = pl.ds(0, geo.kept[stage][0])
        return to(self.s[stage].at[part, rows, :], self.l[stage].at[part, slot, rows, :], self.s_send.at[stage, part],
                  self.s_recv.at[stage, part, slot], self.place.peer[part][stage])

    def send(self, geo, slot, own):
        self.swap0(geo, own, slot).start()

    def first(self, geo, slot, own):
        place = self.place
        copy = self.swap0(geo, own, slot)
        copy.wait_recv()
        for p in BOTH:
            bit = place.bit[p][0]
            base, here = place.core * geo.h0 + p * geo.hp, p * geo.hp

            def add(i):
                return own[rows_of(base + i, STEP), :].astype(F32) + self.l0[slot, rows_of(here + i, STEP), :].astype(F32)

            def give(i):
                self.s[0][p, pl.ds(i, STEP), :] = add((1 - bit) * geo.h1 + i).astype(BF16)

            def keep(i):
                self.k[0][p, pl.ds(i, STEP), :] = add(bit * geo.h1 + i)

            strips(geo.h1, give)
            self.swap(geo, 0, p, slot).start()
            strips(geo.h1, keep)
        copy.wait_send()

    def next(self, geo, stage, slot, q):
        for p in BOTH:
            copy = self.swap(geo, stage, p, slot)
            copy.wait_recv()
            copy.wait_send()
            k, land = self.k[stage], self.l[stage]
            if stage == 3:
                sz, kz = self.items[geo][:2]
                for piece in range(geo.pieces):
                    j = (q * 2 + p) * geo.pieces + piece
                    rows = pl.ds(piece * geo.pr, geo.pr)
                    total = k[p, rows, :] + land[p, slot, rows, :].astype(F32)
                    kz[j] = total
                    sz[j] = total.astype(BF16)
                continue
            bit = self.place.bit[p][stage + 1]

            def add(i, half):
                cols = geo.kept[stage + 1][1]
                at = (rows_of(half * geo.h2 + i, STEP), slice(None)) if stage == 0 else (pl.ds(i, STEP), cols_of(half * cols, cols))
                return k[p, *at] + land[p, slot, *at].astype(F32)

            def give(i):
                self.s[stage + 1][p, pl.ds(i, STEP), :] = add(i, 1 - bit).astype(BF16)

            def keep(i):
                self.k[stage + 1][p, pl.ds(i, STEP), :] = add(i, bit)

            strips(geo.h2, give)
            self.swap(geo, stage + 1, p, slot).start()
            strips(geo.h2, keep)

    def zcopy(self, geo, group, k, landed=""):
        sz, _, lz, send, recv = self.items[geo]
        z = self.place.z
        j = (z + k) % 8
        at = j if landed else z
        return to(sz.at[j], lz.at[group, at], send.at[j], recv.at[group, at], self.place.zpeer(k))

    def over_z(self, geo, group):
        for k in ZS:
            self.zcopy(geo, group, k).start()

    def last(self, geo, group, shard):
        for k in ZS:
            self.zcopy(geo, group, k, landed="yes").wait_recv()
        for k in ZS:
            self.zcopy(geo, group, k).wait_send()
        _, kz, lz = self.items[geo][:3]
        z = self.place.z
        lz[group, z] = jnp.zeros((geo.pr, 128), BF16)
        total = kz[z]
        for j in range(8):
            total = total + lz[group, j].astype(F32)
        shard[...] = total.astype(BF16)


def ag_scratch(chunks, groups):
    dma = pltpu.SemaphoreType.DMA
    return [dma((groups, 8)), dma((groups, 8)), dma((groups,)), dma((5, 2, 2)), dma((5, 2, chunks))]


class AllGather:
    def __init__(self, geo, place, chunks, whole, refs):
        self.geo, self.place, self.n, self.g = geo, place, chunks, whole
        self.z_send, self.z_recv, self.own_sem, self.send, self.recv = refs

    def item(self, group, j):
        g = self.geo
        q, p, piece = j // (2 * g.pieces), (j // g.pieces) % 2, j % g.pieces
        row, _, col = self.place.where(g, p, 2)
        return self.g.at[group * g.nq + q, rows_of(row + piece * g.pr, g.pr), cols_of(col, 128)]

    def zcopy(self, group, shard, k):
        z = self.place.z
        return to(shard, self.item(group, z), self.z_send.at[group, k], self.z_recv.at[group, z], self.place.zpeer(k))

    def own(self, group, shard):
        return pltpu.make_async_copy(shard, self.item(group, self.place.z), self.own_sem.at[group])

    def over_z(self, group, shard):
        self.own(group, shard).start()
        for k in ZS:
            self.zcopy(group, shard, k).start()

    def copy(self, step, c, p):
        g, place = self.geo, self.place
        if step == 4:
            there = self.g.at[c, rows_of(place.core * g.h0, g.h0), :]
            return to(there, there, self.send.at[4, 0, c % 2], self.recv.at[4, 0, c], place.partner)
        row, wide, narrow = place.where(g, p, 2 if step < 3 else 1)
        rows, cols = g.kept[3 - step]
        there = self.g.at[c, rows_of(row, rows), (cols_of(narrow, cols), cols_of(wide, cols), slice(None), slice(None))[step]]
        return to(there, there, self.send.at[step, p, c % 2], self.recv.at[step, p, c], place.peer[p][3 - step])

    def event(self, step, c, shard):
        g, z = self.geo, self.place.z
        if step == 0:
            group = c // g.nq
            for i in range(2 * g.pieces):
                j = (c % g.nq) * 2 * g.pieces + i
                item = self.item(group, j)

                @pl.when(j == z)
                def _():
                    self.own(group, shard(group)).wait()

                @pl.when(j != z)
                def _():
                    to(item, item, self.z_send.at[group, 0], self.z_recv.at[group, j], self.place.partner).wait_recv()
        else:
            for p in BOTH[: 2 - step // 5]:
                self.copy(step - 1, c, p).wait_recv()
        if step == 5:
            return
        parts = BOTH[: 2 - step // 4]

        @pl.when(c >= 2)
        def _():
            for p in parts:
                self.copy(step, c - 2, p).wait_send()

        for p in parts:
            self.copy(step, c, p).start()

    def end(self, shard):
        for c in (self.n - 2, self.n - 1):
            for step in range(5):
                for p in BOTH[: 2 - step // 4]:
                    self.copy(step, c, p).wait_send()
        for group in range(self.n // self.geo.nq):
            for k in ZS:
                self.zcopy(group, shard(group), k).wait_send()


def squares_scratch():
    v, dma = pltpu.VMEM, pltpu.SemaphoreType.DMA
    five, eight = dma((5,)), dma((8,))
    return [v((n, *TILE), F32) for n in (6, 5, 8)] + [five, five, eight, eight]


class Squares:
    def __init__(self, place, refs):
        self.place = place
        self.value, self.land, self.zland, self.send, self.recv, self.z_send, self.z_recv = refs
        self.peers = [place.partner, *place.fixed]

    def swap(self, k):
        return to(self.value.at[k], self.land.at[k], self.send.at[k], self.recv.at[k], self.peers[k])

    def over_z(self, k, landed=""):
        at = (self.place.z + k) % 8 if landed else self.place.z
        return to(self.value.at[5], self.zland.at[at], self.z_send.at[k], self.z_recv.at[at], self.place.zpeer(k))

    def start(self, value):
        self.value[0] = value
        self.swap(0).start()

    def event(self, k, result):
        if k < 5:
            self.swap(k).wait()
            self.value[k + 1] = self.value[k] + self.land[k]
        if k < 4:
            self.swap(k + 1).start()
        elif k == 4:
            self.zland[self.place.z] = self.value[5]
            for i in ZS:
                self.over_z(i).start()
        else:
            for i in ZS:
                self.over_z(i, landed="yes").wait_recv()
            for i in ZS:
                self.over_z(i).wait_send()
            total = self.zland[0]
            for i in ZS:
                total = total + self.zland[i]
            result[...] = total


def _norm(h):
    return lax.rsqrt(_mean(h * h) + 1e-6)


def _turn(t, cos, sin, back=""):
    half = HEAD // 2
    a, b = t[:, :half].astype(F32), t[:, half:].astype(F32)
    if back:
        return jnp.concatenate([a * cos + b * sin, b * cos - a * sin], -1).astype(BF16)
    return jnp.concatenate([a * cos - b * sin, b * cos + a * sin], -1).astype(BF16)


def _hide(scores, value):
    n = scores.shape[0] - QUERIES
    key, query = (lax.broadcasted_iota(jnp.int32, (QUERIES, QUERIES), axis) for axis in BOTH)
    ok = key <= query
    own = jnp.where(ok, scores[n:], value)
    return own if n == 0 else jnp.concatenate([scores[:n], own], 0)


def _attend(x_ref, cos_ref, sin_ref, wq_ref, wk_ref, wv_ref, wo_ref, q_ref, k_ref, v_ref, o_ref, lse_ref, at_ref, h_ref, b_ref, a_s, sum_s):
    head = pl.program_id(0)
    tokens = x_ref.shape[0]

    @pl.when(head == 0)
    def _():
        for i in range(0, tokens, QUERIES):
            x = x_ref[pl.ds(i, QUERIES), :].astype(F32)
            a_s[pl.ds(i, QUERIES), :] = (x * _norm(x)).astype(BF16)
        at_ref[...] = a_s[...].T
        sum_s[...] = jnp.zeros_like(sum_s)

    a = a_s[...]
    q_ref[...] = _turn(_dot(a, wq_ref[0]).astype(BF16), cos_ref[...], sin_ref[...])
    k_ref[...] = _turn(_dot(a, wk_ref[0]).astype(BF16), cos_ref[...], sin_ref[...])
    v_ref[...] = _dot(a, wv_ref[0]).astype(BF16)
    vt = v_ref[...].T
    for i in range(0, tokens, QUERIES):
        n = i + QUERIES
        s = _hide(_dot_t(k_ref[:n, :], q_ref[i:n, :]), HIDDEN)
        top = _down(jnp.max, s)
        p = jnp.exp2((s - top) * (SCALE * LOG2E))
        total = _down(jnp.sum, p)
        o = _dot(vt[:, :n], (p * (1 / total)).astype(BF16))
        o_ref[i:n, :] = o.T.astype(BF16)
        lse_ref[0, :, i:n] = top * (SCALE * LOG2E) + jnp.log2(total)
    sum_s[...] += _dot(o_ref[...], wo_ref[0])

    @pl.when(head == HEADS - 1)
    def _():
        for i in range(0, tokens, QUERIES):
            here = pl.ds(i, QUERIES)
            h = (x_ref[here, :] + sum_s[here, :].astype(BF16)).astype(BF16)
            h_ref[here, :] = h
            wide = h.astype(F32)
            b_ref[here, :] = (wide * _norm(wide)).astype(BF16)


def attend(x, cos, sin, wq, wk, wv, wo):
    tokens, d = x.shape
    fixed = lambda shape: pl.BlockSpec(shape, _origin(shape))
    into, column = pl.BlockSpec((1, d, HEAD), lambda h: (0, 0, h)), pl.BlockSpec((tokens, HEAD), lambda h: (0, h))
    one, lse = jax.ShapeDtypeStruct((tokens, HEADS * HEAD), BF16), (1, 1, tokens)
    states = jax.ShapeDtypeStruct((tokens, d), BF16)
    return pl.pallas_call(
        _attend,
        grid=(HEADS,),
        in_specs=[fixed((tokens, d)), fixed(cos.shape), fixed(sin.shape), into, into, into, pl.BlockSpec((1, HEAD, d), lambda h: (0, h, 0))],
        out_specs=[column] * 4 + [pl.BlockSpec(lse, lambda h: (h, 0, 0)), fixed((d, tokens)), fixed((tokens, d)), fixed((tokens, d))],
        out_shape=[one] * 4 + [jax.ShapeDtypeStruct((HEADS, 1, tokens), F32), jax.ShapeDtypeStruct((d, tokens), BF16), states, states],
        scratch_shapes=[pltpu.VMEM((tokens, d), BF16), pltpu.VMEM((tokens, d), F32)],
        compiler_params=pltpu.CompilerParams(dimension_semantics=("arbitrary",), vmem_limit_bytes=VMEM),
    )(x, cos, sin, wq, wk, wv, wo)


LAST = 25
RS_LAGS = 1, 3, 5, 6, 8, 10
ATT_LAGS = 1, 2, 3, 5, 6
ATT_DONE = 39
GATHER = 0, 2, 4, 7, 10, 12
ATT_GATHER = 1, 3, 4, 5, 7, 8


def _layer(b_ref, dy_ref, h_ref, at_ref, cos_ref, sin_ref, wg_ref, wu_ref, wd_ref, q_ref, k_ref, v_ref, o_ref, lse_ref, wo_ref,
           ffn_ref, att_ref, squares_ref, bt_s, dyt_s, db_s, act_s, dgate_s, dup_s, dk_s, dv_s, own_s, shard_s, mine_s, *refs):
    t = pl.program_id(0)
    place = Place()
    n, m, o = len(rs_scratch()), len(ag_scratch(1, 1)), len(squares_scratch())
    rs = ReduceScatter(place, refs[:n])
    squares = Squares(place, refs[n : n + o])
    ag = AllGather(FFN, place, CHUNKS, ffn_ref, refs[n + o : n + o + m])
    att_ag = AllGather(ATT, place, 2, att_ref, refs[n + o + m :])
    tokens, d = b_ref.shape
    shard, mine = lambda group: shard_s.at[group], lambda group: mine_s

    def own(geo, slot):
        return own_s.at[slot, pl.ds(0, geo.rows), :]

    def chunk(c):
        return (c >= 0) & (c < CHUNKS)

    def sums(half):
        now = 2 * t + half

        def due(lag):
            return [(now - 1 - lag) // 2] if (half - 1 - lag) % 2 == 0 else []

        def attention(lag, event):
            @pl.when((now == 27 + lag) | (now == 31 + lag))
            def _():
                event((now - 27 - lag) // 4)

        for c in due(RS_LAGS[5]):
            @pl.when(chunk(c) & (c % FFN.nq == FFN.nq - 1))
            def _():
                rs.last(FFN, c // FFN.nq, shard_s.at[c // FFN.nq])
                ag.over_z(c // FFN.nq, shard_s.at[c // FFN.nq])

        if half == 1:
            @pl.when(now == ATT_DONE)
            def _():
                rs.last(ATT, 0, mine_s)
                att_ag.over_z(0, mine_s)
                total = jnp.zeros(TILE, F32)
                for ref in (*(shard_s.at[group] for group in range(GROUPS)), mine_s):
                    for i in range(0, ref.shape[0], 16):
                        g = ref[i : i + 16, :].astype(F32)
                        total = total + (g * g).reshape(-1, *TILE).sum(0)
                squares.start(total)

        for stage in reversed(range(4)):
            for c in due(RS_LAGS[stage + 1]):
                @pl.when(chunk(c))
                def _():
                    rs.next(FFN, stage, c % 2, c % FFN.nq)

                if stage == 3:
                    @pl.when(chunk(c) & (c % FFN.nq == FFN.nq - 1))
                    def _():
                        rs.over_z(FFN, c // FFN.nq)

            lag = ATT_LAGS[stage + 1]
            if lag % 2 != half:
                attention(lag, lambda i: rs.next(ATT, stage, i, i))
                if stage == 3:
                    @pl.when(now == 31 + lag)
                    def _():
                        rs.over_z(ATT, 0)

        for c in due(RS_LAGS[0]):
            @pl.when(chunk(c))
            def _():
                rs.first(FFN, c % 2, own(FFN, c % 2))

        if ATT_LAGS[0] % 2 != half:
            attention(ATT_LAGS[0], lambda i: rs.first(ATT, i, own(ATT, i)))

        if half == 1:
            @pl.when(chunk(t))
            def _():
                rs.send(FFN, t % 2, own(FFN, t % 2))

            attention(0, lambda i: rs.send(ATT, i, own(ATT, i)))

        for k in range(6):
            if (ATT_DONE + 1 + k) % 2 == half:
                @pl.when(now == ATT_DONE + 1 + k)
                def _():
                    squares.event(k, squares_ref)

        for step in reversed(range(6)):
            lag = ATT_DONE + ATT_GATHER[step]
            if lag % 2 == half:
                @pl.when(now == lag)
                def _():
                    for c in BOTH:
                        att_ag.event(step, c, mine)

            late = now - GATHER[step]
            if (GATHER[step] + half) % 2 == 1:
                @pl.when((late >= 19) & (late < 32))
                def _():
                    ag.event(step, (late - 19) // 2, shard)

            @pl.when((late >= 34) & (late < 39))
            def _():
                ag.event(step, late - 27, shard)

    @pl.when(t == 0)
    def _():
        greet(place)
        bt_s[...] = b_ref[...].T
        dyt_s[...] = dy_ref[...].T
        db_s[...] = jnp.zeros_like(db_s)

    @pl.when(t < CHUNKS)
    def _():
        wg, wu, wd = wg_ref[0], wu_ref[0], wd_ref[0]
        for i in range(0, tokens, 512):
            here = pl.ds(i, 512)
            gate, up = _dot(b_ref[here, :], wg), _dot(b_ref[here, :], wu)
            dact = _dot_t(dy_ref[here, :], wd).astype(BF16).astype(F32)
            part = 0.5 * jnp.tanh(0.5 * gate) + 0.5
            silu = gate * part
            act_s[here, :] = (silu * up).astype(BF16)
            dup = (dact * silu).astype(BF16)
            dgate = (dact * up * (part + silu * (1.0 - part))).astype(BF16)
            dup_s[here, :] = dup
            dgate_s[here, :] = dgate
            db_s[here, :] += _dot_t(dgate, wg) + _dot_t(dup, wu)

    @pl.when(t == CHUNKS)
    def _():
        for i in range(0, tokens, QUERIES):
            here = pl.ds(i, QUERIES)
            h, g = h_ref[here, :].astype(F32), db_s[here, :].astype(BF16).astype(F32)
            scale = _norm(h)
            back = scale * g - h * (scale * scale * scale * _mean(g * h))
            db_s[here, :] = dy_ref[here, :].astype(F32) + back.astype(BF16).astype(F32)
        bt_s[...] = db_s[...].astype(BF16).T

    def head_columns():
        return cols_of((t % 2) * HEAD, HEAD)

    @pl.when((t >= CHUNKS) & (t < CHUNKS + HEADS))
    def _():
        do_s = act_s.at[:, pl.ds(HEAD, HEAD)]
        dq_s = act_s.at[:, pl.ds(0, HEAD)]
        do_s[...] = _dot_t(db_s[...].astype(BF16), wo_ref[0]).astype(BF16)
        kt = k_ref[...].T
        for i in reversed(range(0, tokens, QUERIES)):
            n = i + QUERIES
            s = _dot_t(k_ref[:n, :], q_ref[i:n, :])
            dp = _dot_t(v_ref[:n, :], do_s[i:n, :])
            p = _hide(jnp.exp2(s * (SCALE * LOG2E) - lse_ref[0, :, i:n]), 0.0)
            ds = (p * (dp - _down(jnp.sum, p * dp))).astype(BF16)
            dv, dk = _dot(p.astype(BF16), do_s[i:n, :]), _dot(ds, q_ref[i:n, :])
            if n == tokens:
                dv_s[...], dk_s[...] = dv, dk
            else:
                dv_s[:n, :] += dv
                dk_s[:n, :] += dk
            dq = (_dot(kt[:, :n], ds) * SCALE).T.astype(BF16)
            dq_s[i:n, :] = _turn(dq, cos_ref[i:n, :], sin_ref[i:n, :], back="yes")
        dgate_s[:, :HEAD] = _turn((dk_s[...] * SCALE).astype(BF16), cos_ref[...], sin_ref[...], back="yes")
        dup_s[:, :HEAD] = dv_s[...].astype(BF16)

    @pl.when(t == 0)
    def _():
        greeted(place)

    sums(0)

    @pl.when(t < CHUNKS)
    def _():
        slot = t % 2
        for i, (left, right) in enumerate(((bt_s, dgate_s), (bt_s, dup_s), (dyt_s, act_s))):
            own_s[slot, i * d : (i + 1) * d, :] = _dot(left[...], right[...]).astype(BF16)

    @pl.when((t >= CHUNKS) & (t < CHUNKS + HEADS))
    def _():
        slot = (t - CHUNKS) // 2
        for i, (left, right) in enumerate(((bt_s, o_ref), (at_ref, act_s), (at_ref, dgate_s), (at_ref, dup_s))):
            own_s[slot, i * d : (i + 1) * d, head_columns()] = _dot(left[...], right[:, :HEAD]).astype(BF16)

    sums(1)

    @pl.when(t == LAST)
    def _():
        ag.end(shard)
        att_ag.end(mine)


def layer(b, dy, h, at, cos, sin, wg, wu, wd, q, k, v, o, lse, wo):
    tokens, d = b.shape
    vm = pltpu.VMEM
    fixed = lambda shape: pl.BlockSpec(shape, _origin(shape), pipeline_mode=pl.Buffered(1))
    step, head = lambda t: jnp.minimum(t, CHUNKS - 1), lambda t: jnp.clip(t - CHUNKS, 0, HEADS - 1)
    into, column = pl.BlockSpec((1, d, BLOCK), lambda t: (0, 0, step(t))), pl.BlockSpec((tokens, HEAD), lambda t: (0, head(t)))
    states, anywhere = fixed((tokens, d)), pl.BlockSpec(memory_space=pl.ANY)
    half = vm((tokens, BLOCK), BF16)
    return pl.pallas_call(
        _layer,
        grid=(LAST + 1,),
        in_specs=[states, states, states, fixed(at.shape), fixed(cos.shape), fixed(sin.shape), into, into,
                  pl.BlockSpec((1, BLOCK, d), lambda t: (0, step(t), 0)), column, column, column, column,
                  pl.BlockSpec((1, 1, tokens), lambda t: (head(t), 0, 0)), pl.BlockSpec((1, HEAD, d), lambda t: (0, head(t), 0))],
        out_specs=[anywhere, anywhere, fixed(TILE)],
        out_shape=[jax.ShapeDtypeStruct((CHUNKS, FFN.rows, WIDE), BF16), jax.ShapeDtypeStruct((2, ATT.rows, WIDE), BF16),
                   jax.ShapeDtypeStruct(TILE, F32)],
        scratch_shapes=[vm((d, tokens), BF16), vm((d, tokens), BF16), vm((tokens, d), F32), half, half, half, vm((tokens, HEAD), F32),
                        vm((tokens, HEAD), F32), vm((2, ATT.rows, WIDE), BF16), vm((GROUPS, FFN.pr, 128), BF16), vm((ATT.pr, 128), BF16),
                        *rs_scratch(), *squares_scratch(), *ag_scratch(CHUNKS, GROUPS), *ag_scratch(2, 1)],
        compiler_params=pltpu.CompilerParams(dimension_semantics=("arbitrary",), vmem_limit_bytes=VMEM, collective_id=1, has_side_effects=True),
    )(b, dy, h, at, cos, sin, wg, wu, wd, q, k, v, o, lse, wo)


def adamw(w, m, v, g):
    m = 0.9 * m + 0.1 * g
    v = 0.95 * v + 0.05 * g * g
    step = m * lax.rsqrt(v + 1e-8) + 0.1 * w
    return (w - 0.02 * step).astype(BF16), m, v


def _adamw(factor_ref, *refs, kinds):
    f = factor_ref[0]
    n = len(kinds)
    given, results = refs[: 4 * n], refs[4 * n :]
    for i, transposed in enumerate(kinds):
        w_ref, m_ref, v_ref, g_ref = given[4 * i : 4 * i + 4]
        g = g_ref[0].astype(F32)
        new = adamw(w_ref[0].astype(F32), m_ref[0], v_ref[0], (g.T if transposed else g) * f)
        for ref, value in zip(results[3 * i : 3 * i + 3], new, strict=True):
            ref[0] = value


def update(factor, weights, m, v, whole, first, last, grid):
    in_specs, args, out_specs, shapes = [pl.BlockSpec(memory_space=pltpu.SMEM)], [factor], [], []
    for n, (w, m_, v_) in enumerate(zip(weights, m, v, strict=True)):
        spec = pl.BlockSpec((1, 512, 256), lambda i, j: (0, i, j)) if n == last else pl.BlockSpec((1, 256, 512), lambda i, j: (0, j, i))
        in_specs += [spec, spec, spec, pl.BlockSpec((1, 256, 512), lambda i, j, at=first[n]: (i, at + j, 0))]
        args += [w, m_, v_, whole]
        out_specs += [spec] * 3
        shapes += [jax.ShapeDtypeStruct(w.shape, t) for t in (BF16, F32, F32)]
    out = pl.pallas_call(
        functools.partial(_adamw, kinds=[n == last for n in range(len(weights))]),
        grid=grid,
        in_specs=in_specs,
        out_specs=out_specs,
        out_shape=shapes,
        compiler_params=pltpu.CompilerParams(dimension_semantics=("arbitrary",) * len(grid), vmem_limit_bytes=VMEM),
    )(*args)
    return [out[i::3] for i in range(3)]


def solution(mesh):
    def step(x, dy, *arrays):
        weights, m, v = (arrays[i : i + 7] for i in (0, 7, 14))
        wq, wk, wv, wo, wg, wu, wd = weights
        half = HEAD // 2
        angle = jnp.arange(x.shape[1], dtype=F32)[:, None] * THETA ** (-jnp.arange(half, dtype=F32) / half)
        cos, sin = jnp.cos(angle), jnp.sin(angle)
        q, k, v_, o, lse, at, h, b = attend(x[0], cos, sin, wq, wk, wv, wo)
        ffn_g, att_g, squares = layer(b, dy[0], h, at, cos, sin, wg, wu, wd, q, k, v_, o, lse, wo)
        count = sum(w.size for w in weights)
        factor = jnp.minimum(1.0, 0.5 * lax.rsqrt(jnp.sum(squares) / count + 1e-30)).reshape(1)
        ffn = update(factor, weights[4:], m[4:], v[4:], ffn_g, (0, 3, 6), 2, (CHUNKS, 3))
        att = update(factor, weights[:4], m[:4], v[:4], att_g, (3, 6, 9, 0), 3, (2, 3))
        return tuple(one for a, f in zip(att, ffn, strict=True) for one in (*a, *f))

    states, all_of = P(("rep", "dp"), None, None), P(None, None, None)
    return jax.shard_map(
        step,
        mesh=mesh,
        in_specs=(states, states) + (all_of,) * 21,
        out_specs=(P("rep", None, None),) * 21,
        check_vma=False,
    )
```

```python
import functools

import jax
import jax.numpy as jnp
import numpy as np
from jax import lax
from jax.experimental import pallas as pl
from jax.experimental.pallas import tpu as pltpu
from jax.sharding import PartitionSpec as P

MESH = pl.DeviceIdType.MESH
F32, BF16 = jnp.float32, jnp.bfloat16
VMEM = 61 * 2**20
HEAD = 256
HALF = HEAD // 2
THETA = 10000
LOG2E = 1.4426950408889634
SCALE = HEAD**-0.5
HIDDEN = -1e30
WIDE = 512
MIDDLE = WIDE // 2
LANES = 128
TILE = (8, LANES)
ZS = range(1, 8)
BOTH = range(2)
STEP = 48
BLOCK = WIDE
CHUNKS = 12
HEADS = 4
QUERIES = HEAD


def _dot(a, b):
    return jnp.dot(a, b, preferred_element_type=F32)


def _dot_t(a, b):
    return lax.dot_general(a, b, (((1,), (1,)), ((), ())), preferred_element_type=F32)


def rem(a, b):
    return a % b if isinstance(a, int) else lax.rem(a, jnp.int32(b))


def div(a, b):
    return a // b if isinstance(a, int) else lax.div(a, jnp.int32(b))


def whole(ref):
    return ref[...]


def put(ref, value):
    ref[...] = value


def one(ref):
    return ref[0]


def blocks(tokens):
    return range(0, tokens, QUERIES)


def _down(reduce, x):
    return reduce(x, 0, keepdims=True)


def _mean(x):
    return jnp.mean(x, -1, keepdims=True)


def _origin(shape):
    return lambda _: (0,) * len(shape)


def mix(bit, if0, if1):
    return if0 * (1 - bit) + if1 * bit


class Geo:
    def __init__(self, rows, per_group):
        self.rows, self.nq = rows, per_group
        self.h0, self.hp, self.h1, self.h2 = rows // 2, rows // 4, rows // 8, rows // 16
        self.pieces = 4 // per_group
        self.pr = self.h2 // self.pieces
        self.kept = (self.h1, WIDE), (self.h2, WIDE), (self.h2, 256), (self.h2, LANES)


FFN, ATT = Geo(2304, 4), Geo(3072, 2)
GROUPS = CHUNKS // FFN.nq
EARLY = 8
LATE = (CHUNKS - EARLY) * FFN.h1


class Place:
    def __init__(self):
        d = lax.axis_index("dp")
        core, z, y, x = rem(d, 2), rem(div(d, 2), 8), rem(div(d, 16), 4), div(d, 64)
        self.core, self.z = core, z
        at = lambda x, y, z, core: ((x * 4 + y) * 8 + z) * 2 + core
        other = lambda c, kind: c + 1 - 2 * rem(c, 2) if kind == 1 else 3 - c
        half = lambda c, kind: rem(div(c + 1, 2), 2) if kind == 1 else div(c, 2)
        swap = {("x", k): (at(other(x, k), y, z, core), half(x, k)) for k in (1, 3)}
        swap.update({("y", k): (at(x, other(y, k), z, core), half(y, k)) for k in (1, 3)})
        order = ("x", 1), ("x", 3), ("y", 1), ("y", 3)
        self.fixed = [swap[key][0] for key in order]
        both = [[(swap[a, k], swap[a, 4 - k]) for a, k in keys] for keys in (order, order[::-1])]
        self.peer = [[mix(core, one[0], two[0]) for one, two in part] for part in both]
        self.bit = [[mix(core, one[1], two[1]) for one, two in part] for part in both]
        self.other = [mix(core, part[0][1][1], part[0][0][1]) for part in both]
        self.partner = at(x, y, z, 1 - core)
        self.zpeer = lambda k: at(x, y, rem(z + k, 8), core)
        self.all_peers = [self.partner, *self.fixed, *(self.zpeer(k) for k in ZS)]

    def inside(self, geo, p):
        b = self.bit[p]
        return b[1] * geo.h2, b[2] * MIDDLE, b[2] * MIDDLE + b[3] * LANES


def rep_index():
    return lax.axis_index("rep")


def to(src, dst, send, recv, device):
    return pltpu.make_async_remote_copy(src_ref=src, dst_ref=dst, send_sem=send, recv_sem=recv, device_id=(rep_index(), device),
                                        device_id_type=MESH)


def greet(place):
    barrier = pltpu.get_barrier_semaphore()
    for peer in place.all_peers:
        pl.semaphore_signal(barrier, inc=1, device_id=(rep_index(), peer), device_id_type=MESH)


def greeted(place):
    pl.semaphore_wait(pltpu.get_barrier_semaphore(), len(place.all_peers))


def rows_of(start, size):
    return pl.ds(pl.multiple_of(start, 16), size)


def cols_of(start, size):
    return pl.ds(pl.multiple_of(start, LANES), size)


def strips(rows, body):
    lax.fori_loop(0, rows // STEP, lambda i, _: body(pl.multiple_of(i * STEP, STEP)), None)


def rs_scratch():
    v, dma = pltpu.VMEM, pltpu.SemaphoreType.DMA
    out = [v((2, ATT.h0, WIDE), BF16), dma((1,)), dma((2,)), dma((4, 2)), dma((4, 2, 2))]
    for kept in ATT.kept:
        out += [v((2, *kept), BF16), v((2, *kept), F32), v((2, 2, *kept), BF16)]
    for geo, groups in ((FFN, GROUPS), (ATT, 1)):
        out += [v((8, geo.pr, LANES), BF16), v((8, geo.pr, LANES), F32), v((groups, 8, geo.pr, LANES), BF16), dma((8,)), dma((groups, 8))]
    return out


class ReduceScatter:
    def __init__(self, place, refs):
        self.place = place
        self.l0, self.d_send, self.d_recv, self.s_send, self.s_recv = refs[:5]
        swaps, items = refs[5:17], refs[17:]
        self.s, self.k, self.l = swaps[0::3], swaps[1::3], swaps[2::3]
        self.items = {FFN: items[:5], ATT: items[5:]}

    def swap0(self, geo, own, slot):
        return to(own.at[rows_of((1 - self.place.core) * geo.h0, geo.h0), :], self.l0.at[slot, pl.ds(0, geo.h0), :], self.d_send.at[0],
                  self.d_recv.at[slot], self.place.partner)

    def swap(self, geo, stage, part, slot):
        rows = pl.ds(0, geo.kept[stage][0])
        return to(self.s[stage].at[part, rows, :], self.l[stage].at[part, slot, rows, :], self.s_send.at[stage, part],
                  self.s_recv.at[stage, part, slot], self.place.peer[part][stage])

    def send(self, geo, slot, own):
        self.swap0(geo, own, slot).start()

    def first(self, geo, slot, own):
        place = self.place
        copy = self.swap0(geo, own, slot)
        copy.wait_recv()
        for p in BOTH:
            bit = place.bit[p][0]
            base, here = place.core * geo.h0 + p * geo.hp, p * geo.hp

            def add(i):
                return own[rows_of(base + i, STEP), :].astype(F32) + self.l0[slot, rows_of(here + i, STEP), :].astype(F32)

            def give(i):
                self.s[0][p, pl.ds(i, STEP), :] = add((1 - bit) * geo.h1 + i).astype(BF16)

            def keep(i):
                self.k[0][p, pl.ds(i, STEP), :] = add(bit * geo.h1 + i)

            strips(geo.h1, give)
            self.swap(geo, 0, p, slot).start()
            strips(geo.h1, keep)
        copy.wait_send()

    def next(self, geo, stage, slot, q):
        for p in BOTH:
            copy = self.swap(geo, stage, p, slot)
            copy.wait_recv()
            copy.wait_send()
            k, land = self.k[stage], self.l[stage]
            if stage == 3:
                sz, kz = self.items[geo][:2]
                for piece in range(geo.pieces):
                    j = (q * 2 + p) * geo.pieces + piece
                    rows = pl.ds(piece * geo.pr, geo.pr)
                    total = k[p, rows, :] + land[p, slot, rows, :].astype(F32)
                    kz[j] = total
                    sz[j] = total.astype(BF16)
                continue
            bit = self.place.bit[p][stage + 1]

            def add(i, half):
                cols = geo.kept[stage + 1][1]
                at = (rows_of(half * geo.h2 + i, STEP), slice(None)) if stage == 0 else (pl.ds(i, STEP), cols_of(half * cols, cols))
                return k[p, *at] + land[p, slot, *at].astype(F32)

            def give(i):
                self.s[stage + 1][p, pl.ds(i, STEP), :] = add(i, 1 - bit).astype(BF16)

            def keep(i):
                self.k[stage + 1][p, pl.ds(i, STEP), :] = add(i, bit)

            strips(geo.h2, give)
            self.swap(geo, stage + 1, p, slot).start()
            strips(geo.h2, keep)

    def zcopy(self, geo, group, k, landed=""):
        sz, _, lz, send, recv = self.items[geo]
        z = self.place.z
        j = rem(z + k, 8)
        at = j if landed else z
        return to(sz.at[j], lz.at[group, at], send.at[j], recv.at[group, at], self.place.zpeer(k))

    def over_z(self, geo, group):
        for k in ZS:
            self.zcopy(geo, group, k).start()

    def last(self, geo, group, shard):
        for k in ZS:
            self.zcopy(geo, group, k, landed="yes").wait_recv()
        for k in ZS:
            self.zcopy(geo, group, k).wait_send()
        _, kz, lz = self.items[geo][:3]
        z = self.place.z
        lz[group, z] = jnp.zeros((geo.pr, LANES), BF16)
        total = kz[z]
        for j in range(8):
            total = total + lz[group, j].astype(F32)
        put(shard, total.astype(BF16))


def ag_scratch(chunks, groups):
    dma = pltpu.SemaphoreType.DMA
    return [dma((groups, 8)), dma((groups, 8)), dma((groups,)), dma((5, 2, 2)), dma((5, 2, chunks))]


class AllGather:
    def __init__(self, geo, place, chunks, target, refs, base=""):
        self.geo, self.place, self.n, self.g, self.base = geo, place, chunks, target, base
        self.late = base != ""
        self.z_send, self.z_recv, self.own_sem, self.send, self.recv = refs

    def region(self, p, c, row, rows, cols):
        g = self.geo
        if self.late:
            return self.g[p].at[rows_of(self.base + c * g.h1 + row, rows), cols]
        return self.g.at[c, rows_of(self.place.core * g.h0 + p * g.hp + self.place.bit[p][0] * g.h1 + row, rows), cols]

    def item(self, p, c, piece):
        row, _, col = self.place.inside(self.geo, p)
        return self.region(p, c, row + piece * self.geo.pr, self.geo.pr, cols_of(col, LANES))

    def zcopy(self, group, shard, k, target):
        return to(shard, target, self.z_send.at[group, k], self.z_recv.at[group, self.place.z], self.place.zpeer(k))

    def over_z(self, group, shard):
        g, z = self.geo, self.place.z
        for p in BOTH:
            @pl.when(rem(div(z, g.pieces), 2) == p)
            def _(p=p):
                target = self.item(p, group * g.nq + div(z, 2 * g.pieces), rem(z, g.pieces))
                pltpu.make_async_copy(shard, target, self.own_sem.at[group]).start()
                for k in ZS:
                    self.zcopy(group, shard, k, target).start()

    def copy(self, step, c, p):
        g, place = self.geo, self.place
        if step == 4:
            there = self.g.at[c, rows_of(place.core * g.h0, g.h0), :]
            return to(there, there, self.send.at[4, 0, rem(c, 2)], self.recv.at[4, 0, c], place.partner)
        row, wide, narrow = place.inside(g, p)
        rows, cols = g.kept[3 - step]
        there = self.region(p, c, row if step < 3 else 0, rows, (cols_of(narrow, cols), cols_of(wide, cols), slice(None), slice(None))[step])
        return to(there, there, self.send.at[step, p, rem(c, 2)], self.recv.at[step, p, c], place.peer[p][3 - step])

    def event(self, step, c, shard):
        g, z = self.geo, self.place.z
        ends = 3 if self.late else 5
        if step == 0:
            group = div(c, g.nq)
            for i in range(2 * g.pieces):
                j = (c - group * g.nq) * 2 * g.pieces + i
                item = self.item(i // g.pieces, c, i % g.pieces)

                @pl.when(j == z)
                def _():
                    pltpu.make_async_copy(shard(group), item, self.own_sem.at[group]).wait()

                @pl.when(j != z)
                def _():
                    to(item, item, self.z_send.at[group, 0], self.z_recv.at[group, j], self.place.partner).wait_recv()
        else:
            for p in BOTH[: 2 - step // 5]:
                self.copy(step - 1, c, p).wait_recv()
        if step == ends:
            return
        parts = BOTH[: 2 - step // 4]

        @pl.when(c >= 2)
        def _():
            for p in parts:
                self.copy(step, c - 2, p).wait_send()

        for p in parts:
            self.copy(step, c, p).start()

    def end(self, shard):
        for c in (self.n - 2, self.n - 1):
            for step in range(3 if self.late else 5):
                for p in BOTH[: 2 - step // 4]:
                    self.copy(step, c, p).wait_send()
        for group in range(self.n // self.geo.nq):
            for k in ZS:
                self.zcopy(group, shard(group), k, self.item(0, 0, 0)).wait_send()


def squares_scratch():
    v, dma = pltpu.VMEM, pltpu.SemaphoreType.DMA
    five, eight = dma((5,)), dma((8,))
    return [v((n, *TILE), F32) for n in (6, 5, 8)] + [five, five, eight, eight]


class Squares:
    def __init__(self, place, refs):
        self.place = place
        self.value, self.land, self.zland, self.send, self.recv, self.z_send, self.z_recv = refs
        self.peers = [place.partner, *place.fixed]

    def swap(self, k):
        return to(self.value.at[k], self.land.at[k], self.send.at[k], self.recv.at[k], self.peers[k])

    def over_z(self, k, landed=""):
        at = rem(self.place.z + k, 8) if landed else self.place.z
        return to(self.value.at[5], self.zland.at[at], self.z_send.at[k], self.z_recv.at[at], self.place.zpeer(k))

    def start(self, value):
        self.value[0] = value
        self.swap(0).start()

    def event(self, k, result):
        if k < 5:
            self.swap(k).wait()
            self.value[k + 1] = self.value[k] + self.land[k]
        if k < 4:
            self.swap(k + 1).start()
        elif k == 4:
            self.zland[self.place.z] = self.value[5]
            for i in ZS:
                self.over_z(i).start()
        else:
            for i in ZS:
                self.over_z(i, landed="yes").wait_recv()
            for i in ZS:
                self.over_z(i).wait_send()
            total = self.zland[0]
            for i in ZS:
                total = total + self.zland[i]
            put(result, total)


def _norm(h):
    return lax.rsqrt(_mean(h * h) + 1e-6)


def _turn(t, cos, sin, back=""):
    half = HALF
    a, b = t[:, :half].astype(F32), t[:, half:].astype(F32)
    if back:
        return jnp.concatenate([a * cos + b * sin, b * cos - a * sin], -1).astype(BF16)
    return jnp.concatenate([a * cos - b * sin, b * cos + a * sin], -1).astype(BF16)


def _hide(scores, value):
    n = scores.shape[0] - QUERIES
    key, query = (lax.broadcasted_iota(jnp.int32, (QUERIES, QUERIES), axis) for axis in BOTH)
    ok = key <= query
    own = jnp.where(ok, scores[n:], value)
    return own if n == 0 else jnp.concatenate([scores[:n], own], 0)


def _attend(x_ref, cos_ref, sin_ref, wq_ref, wk_ref, wv_ref, wo_ref, q_ref, k_ref, v_ref, o_ref, lse_ref, at_ref, h_ref, b_ref, a_s, sum_s):
    head = pl.program_id(0)
    tokens = x_ref.shape[0]

    @pl.when(head == 0)
    def _():
        for i in blocks(tokens):
            x = x_ref[pl.ds(i, QUERIES), :].astype(F32)
            a_s[pl.ds(i, QUERIES), :] = (x * _norm(x)).astype(BF16)
        put(at_ref, whole(a_s).T)
        put(sum_s, jnp.zeros_like(sum_s))

    a = whole(a_s)
    put(q_ref, _turn(_dot(a, one(wq_ref)).astype(BF16), whole(cos_ref), whole(sin_ref)))
    put(k_ref, _turn(_dot(a, one(wk_ref)).astype(BF16), whole(cos_ref), whole(sin_ref)))
    put(v_ref, _dot(a, one(wv_ref)).astype(BF16))
    vt = whole(v_ref).T
    for i in blocks(tokens):
        n = i + QUERIES
        s = _hide(_dot_t(k_ref[:n, :], q_ref[i:n, :]), HIDDEN)
        top = _down(jnp.max, s)
        p = jnp.exp2((s - top) * (SCALE * LOG2E))
        total = _down(jnp.sum, p)
        o = _dot(vt[:, :n], (p * (1 / total)).astype(BF16))
        o_ref[i:n, :] = o.T.astype(BF16)
        lse_ref[0, :, i:n] = top * (SCALE * LOG2E) + jnp.log2(total)
    put(sum_s, whole(sum_s) + _dot(whole(o_ref), one(wo_ref)))

    @pl.when(head == HEADS - 1)
    def _():
        for i in blocks(tokens):
            here = pl.ds(i, QUERIES)
            h = (x_ref[here, :] + sum_s[here, :].astype(BF16)).astype(BF16)
            h_ref[here, :] = h
            wide = h.astype(F32)
            b_ref[here, :] = (wide * _norm(wide)).astype(BF16)


def attend(x, cos, sin, wq, wk, wv, wo):
    tokens, d = x.shape
    fixed = lambda shape: pl.BlockSpec(shape, _origin(shape))
    into, column = pl.BlockSpec((1, d, HEAD), lambda h: (0, 0, h)), pl.BlockSpec((tokens, HEAD), lambda h: (0, h))
    one, lse = jax.ShapeDtypeStruct((tokens, HEADS * HEAD), BF16), (1, 1, tokens)
    states = jax.ShapeDtypeStruct((tokens, d), BF16)
    return pl.pallas_call(
        _attend,
        grid=(HEADS,),
        in_specs=[fixed((tokens, d)), fixed(cos.shape), fixed(sin.shape), into, into, into, pl.BlockSpec((1, HEAD, d), lambda h: (0, h, 0))],
        out_specs=[column] * 4 + [pl.BlockSpec(lse, lambda h: (h, 0, 0)), fixed((d, tokens)), fixed((tokens, d)), fixed((tokens, d))],
        out_shape=[one] * 4 + [jax.ShapeDtypeStruct((HEADS, 1, tokens), F32), jax.ShapeDtypeStruct((d, tokens), BF16), states, states],
        scratch_shapes=[pltpu.VMEM((tokens, d), BF16), pltpu.VMEM((tokens, d), F32)],
        compiler_params=pltpu.CompilerParams(dimension_semantics=("arbitrary",), vmem_limit_bytes=VMEM),
    )(x, cos, sin, wq, wk, wv, wo)


LAST = 22
RS_LAGS = 1, 3, 5, 6, 8, 10
ATT_LAGS = 1, 2, 3, 5, 6
ATT_DONE = 39
GATHER = 0, 2, 4, 7, 10, 12
ATT_GATHER = 1, 2, 4, 5


def _layer(b_ref, dy_ref, h_ref, at_ref, cos_ref, sin_ref, wg_ref, wu_ref, wd_ref, q_ref, k_ref, v_ref, o_ref, lse_ref, wo_ref,
           early_ref, late0_ref, late1_ref, squares_ref, bt_s, dyt_s, db_s, act_s, dgate_s, dup_s, dk_s, dv_s, own_s, shard_s, mine_s, *refs):
    t = pl.program_id(0)
    place = Place()
    n, m, o = len(rs_scratch()), len(ag_scratch(1, 1)), len(squares_scratch())
    rs = ReduceScatter(place, refs[:n])
    squares = Squares(place, refs[n : n + o])
    late = late0_ref, late1_ref
    ag = AllGather(FFN, place, EARLY, early_ref, refs[n + o : n + o + m])
    late_ag = AllGather(FFN, place, CHUNKS - EARLY, late, refs[n + o + m : n + o + 2 * m], base=0)
    att_ag = AllGather(ATT, place, 2, late, refs[n + o + 2 * m :], base=LATE)
    tokens, d = b_ref.shape
    shard, late_shard, mine = lambda group: shard_s.at[group], lambda group: shard_s.at[GROUPS - 1], lambda group: mine_s

    def own(geo, slot):
        return own_s.at[slot, pl.ds(0, geo.rows), :]

    def chunk(c):
        return (c >= 0) & (c < CHUNKS)

    def sums(half):
        now = 2 * t + half

        def due(lag):
            return [t + (half - 1 - lag) // 2] if (half - 1 - lag) % 2 == 0 else []

        def attention(lag, event):
            @pl.when((now == 27 + lag) | (now == 31 + lag))
            def _():
                event((now == 31 + lag).astype(jnp.int32))

        for c in due(RS_LAGS[5]):
            @pl.when(chunk(c) & (rem(c, FFN.nq) == FFN.nq - 1))
            def _():
                rs.last(FFN, div(c, FFN.nq), shard_s.at[div(c, FFN.nq)])

            @pl.when((c >= 0) & (c < EARLY) & (rem(c, FFN.nq) == FFN.nq - 1))
            def _():
                ag.over_z(div(c, FFN.nq), shard_s.at[div(c, FFN.nq)])

            @pl.when(c == CHUNKS - 1)
            def _():
                late_ag.over_z(0, late_shard(0))

        if half == 1:
            @pl.when(now == ATT_DONE)
            def _():
                rs.last(ATT, 0, mine_s)
                att_ag.over_z(0, mine_s)
                total = jnp.zeros(TILE, F32)
                for ref in (*(shard_s.at[group] for group in range(GROUPS)), mine_s):
                    for i in range(0, ref.shape[0], 16):
                        g = ref[i : i + 16, :].astype(F32)
                        total = total + (g * g).reshape(-1, *TILE).sum(0)
                squares.start(total)

        for stage in reversed(range(4)):
            for c in due(RS_LAGS[stage + 1]):
                @pl.when(chunk(c))
                def _():
                    rs.next(FFN, stage, rem(c, 2), rem(c, FFN.nq))

                if stage == 3:
                    @pl.when(chunk(c) & (rem(c, FFN.nq) == FFN.nq - 1))
                    def _():
                        rs.over_z(FFN, div(c, FFN.nq))

            lag = ATT_LAGS[stage + 1]
            if lag % 2 != half:
                attention(lag, lambda i: rs.next(ATT, stage, i, i))
                if stage == 3:
                    @pl.when(now == 31 + lag)
                    def _():
                        rs.over_z(ATT, 0)

        for c in due(RS_LAGS[0]):
            @pl.when(chunk(c))
            def _():
                rs.first(FFN, rem(c, 2), own(FFN, rem(c, 2)))

        if ATT_LAGS[0] % 2 != half:
            attention(ATT_LAGS[0], lambda i: rs.first(ATT, i, own(ATT, i)))

        if half == 1:
            @pl.when(chunk(t))
            def _():
                rs.send(FFN, rem(t, 2), own(FFN, rem(t, 2)))

            attention(0, lambda i: rs.send(ATT, i, own(ATT, i)))

        for k in range(6):
            if (ATT_DONE + 1 + k) % 2 == half:
                @pl.when(now == ATT_DONE + 1 + k)
                def _():
                    squares.event(k, squares_ref)

        for step in reversed(range(6)):
            if step < 4:
                lag = ATT_DONE + ATT_GATHER[step]
                if lag % 2 == half:
                    @pl.when(now == lag)
                    def _():
                        for c in BOTH:
                            att_ag.event(step, c, mine)

            since = now - GATHER[step]
            if (GATHER[step] + half) % 2 == 1:
                @pl.when((since >= 19) & (since < 19 + 2 * EARLY))
                def _():
                    ag.event(step, t + (half - GATHER[step] - 19) // 2, shard)

            if step < 4:
                @pl.when((since >= 35) & (since < 39))
                def _():
                    late_ag.event(step, since - 35, late_shard)

    @pl.when(t == 0)
    def _():
        greet(place)
        put(bt_s, whole(b_ref).T)
        put(dyt_s, whole(dy_ref).T)
        put(db_s, jnp.zeros_like(db_s))

    @pl.when(t < CHUNKS)
    def _():
        wg, wu, wd = (one(ref) for ref in (wg_ref, wu_ref, wd_ref))
        for i in range(0, tokens, WIDE):
            here = pl.ds(i, WIDE)
            gate, up = _dot(b_ref[here, :], wg), _dot(b_ref[here, :], wu)
            dact = _dot_t(dy_ref[here, :], wd).astype(BF16).astype(F32)
            part = 0.5 * jnp.tanh(0.5 * gate) + 0.5
            silu = gate * part
            act_s[here, :] = (silu * up).astype(BF16)
            dup = (dact * silu).astype(BF16)
            dgate = (dact * up * (part + silu * (1.0 - part))).astype(BF16)
            dup_s[here, :] = dup
            dgate_s[here, :] = dgate
            db_s[here, :] += _dot_t(dgate, wg) + _dot_t(dup, wu)

    @pl.when(t == CHUNKS)
    def _():
        for i in blocks(tokens):
            here = pl.ds(i, QUERIES)
            h, g = h_ref[here, :].astype(F32), db_s[here, :].astype(BF16).astype(F32)
            scale = _norm(h)
            back = scale * g - h * (scale * scale * scale * _mean(g * h))
            db_s[here, :] = dy_ref[here, :].astype(F32) + back.astype(BF16).astype(F32)
        put(bt_s, whole(db_s).astype(BF16).T)

    def head_columns():
        return cols_of(rem(t, 2) * HEAD, HEAD)

    @pl.when((t >= CHUNKS) & (t < CHUNKS + HEADS))
    def _():
        do_s = act_s.at[:, pl.ds(HEAD, HEAD)]
        dq_s = act_s.at[:, pl.ds(0, HEAD)]
        put(do_s, _dot_t(whole(db_s).astype(BF16), one(wo_ref)).astype(BF16))
        kt = whole(k_ref).T
        for i in reversed(blocks(tokens)):
            n = i + QUERIES
            s = _dot_t(k_ref[:n, :], q_ref[i:n, :])
            dp = _dot_t(v_ref[:n, :], do_s[i:n, :])
            p = _hide(jnp.exp2(s * (SCALE * LOG2E) - lse_ref[0, :, i:n]), 0.0)
            ds = (p * (dp - _down(jnp.sum, p * dp))).astype(BF16)
            dv, dk = _dot(p.astype(BF16), do_s[i:n, :]), _dot(ds, q_ref[i:n, :])
            if n == tokens:
                put(dv_s, dv)
                put(dk_s, dk)
            else:
                dv_s[:n, :] += dv
                dk_s[:n, :] += dk
            dq = (_dot(kt[:, :n], ds) * SCALE).T.astype(BF16)
            dq_s[i:n, :] = _turn(dq, cos_ref[i:n, :], sin_ref[i:n, :], back="yes")
        dgate_s[:, :HEAD] = _turn((whole(dk_s) * SCALE).astype(BF16), whole(cos_ref), whole(sin_ref), back="yes")
        dup_s[:, :HEAD] = whole(dv_s).astype(BF16)

    @pl.when(t == 0)
    def _():
        greeted(place)

    sums(0)

    @pl.when(t < CHUNKS)
    def _():
        slot = rem(t, 2)
        for i, (left, right) in enumerate(((bt_s, dgate_s), (bt_s, dup_s), (dyt_s, act_s))):
            own_s[slot, i * d : (i + 1) * d, :] = _dot(whole(left), whole(right)).astype(BF16)

    @pl.when((t >= CHUNKS) & (t < CHUNKS + HEADS))
    def _():
        slot = div(t - CHUNKS, 2)
        for i, (left, right) in enumerate(((bt_s, o_ref), (at_ref, act_s), (at_ref, dgate_s), (at_ref, dup_s))):
            own_s[slot, i * d : (i + 1) * d, head_columns()] = _dot(whole(left), right[:, :HEAD]).astype(BF16)

    sums(1)

    @pl.when(t == LAST)
    def _():
        ag.end(shard)
        late_ag.end(late_shard)
        att_ag.end(mine)


def layer(b, dy, h, at, cos, sin, wg, wu, wd, q, k, v, o, lse, wo):
    tokens, d = b.shape
    vm = pltpu.VMEM
    fixed = lambda shape: pl.BlockSpec(shape, _origin(shape), pipeline_mode=pl.Buffered(1))
    step, head = lambda t: jnp.minimum(t, CHUNKS - 1), lambda t: jnp.clip(t - CHUNKS, 0, HEADS - 1)
    into, column = pl.BlockSpec((1, d, BLOCK), lambda t: (0, 0, step(t))), pl.BlockSpec((tokens, HEAD), lambda t: (0, head(t)))
    states, anywhere = fixed((tokens, d)), pl.BlockSpec(memory_space=pl.ANY)
    half, late = vm((tokens, BLOCK), BF16), jax.ShapeDtypeStruct((LATE + 2 * ATT.h1, WIDE), BF16)
    return pl.pallas_call(
        _layer,
        grid=(LAST + 1,),
        in_specs=[states, states, states, fixed(at.shape), fixed(cos.shape), fixed(sin.shape), into, into,
                  pl.BlockSpec((1, BLOCK, d), lambda t: (0, step(t), 0)), column, column, column, column,
                  pl.BlockSpec((1, 1, tokens), lambda t: (head(t), 0, 0)), pl.BlockSpec((1, HEAD, d), lambda t: (0, head(t), 0))],
        out_specs=[anywhere, anywhere, anywhere, fixed(TILE)],
        out_shape=[jax.ShapeDtypeStruct((EARLY, FFN.rows, WIDE), BF16), late, late, jax.ShapeDtypeStruct(TILE, F32)],
        scratch_shapes=[vm((d, tokens), BF16), vm((d, tokens), BF16), vm((tokens, d), F32), half, half, half, vm((tokens, HEAD), F32),
                        vm((tokens, HEAD), F32), vm((2, ATT.rows, WIDE), BF16), vm((GROUPS, FFN.pr, LANES), BF16), vm((ATT.pr, LANES), BF16),
                        *rs_scratch(), *squares_scratch(), *ag_scratch(EARLY, GROUPS - 1), *ag_scratch(CHUNKS - EARLY, 1), *ag_scratch(2, 1)],
        compiler_params=pltpu.CompilerParams(dimension_semantics=("arbitrary",), vmem_limit_bytes=VMEM, collective_id=1, has_side_effects=True),
    )(b, dy, h, at, cos, sin, wg, wu, wd, q, k, v, o, lse, wo)


def adamw(w, m, v, g):
    m = 0.9 * m + 0.1 * g
    v = 0.95 * v + 0.05 * g * g
    step = m * lax.rsqrt(v + 1e-8) + 0.1 * w
    return (w - 0.02 * step).astype(BF16), m, v


TALL, FLAT = (768, WIDE), (WIDE, 768)
RING = {TALL: 6, FLAT: 3}


def _blocks(late):
    for c in range(EARLY, CHUNKS) if late else range(EARLY):
        yield from ((TALL, 4, c, FFN, c, 0), (TALL, 5, c, FFN, c, 1), (FLAT, 6, c, FFN, c, 2))
    if late:
        for i in BOTH:
            yield from ((TALL, 0, i, ATT, i, 1), (TALL, 1, i, ATT, i, 2), (FLAT, 3, i, ATT, i, 0), (TALL, 2, i, ATT, i, 3))


def _update(squares_ref, *refs, late):
    sources, refs = refs[: 8 if late else 1], refs[8 if late else 1 :]
    given, results, buffers = refs[:21], refs[-33:-12], refs[-12:]
    rings = {TALL: buffers[:6], FLAT: buffers[6:]}
    count = sum(ref.size for ref in given[:7])
    factor = jnp.minimum(1.0, 0.5 * lax.rsqrt(jnp.sum(whole(squares_ref)) / count + 1e-30))
    place = Place()

    def gradient(geo, chunk, rows, target, sem, start):
        top = rows * 768
        if not late:
            copy = pltpu.make_async_copy(sources[0].at[chunk, pl.ds(top, 768)], target, sem.at[3])
            copy.start() if start else copy.wait()
            return
        base = (chunk - EARLY) * geo.h1 if geo is FFN else LATE + chunk * geo.h1
        for i, r in enumerate(range(top // geo.h1, -(-(top + 768) // geo.h1))):
            first, end = max(top, r * geo.h1), min(top + 768, (r + 1) * geo.h1)
            core, p, half = r // 4, r // 2 % 2, r % 2
            own = place.core == core
            kept = jnp.where(own, place.bit[p][0], place.other[p]) == half
            part = target.at[pl.ds(first - top, end - first)]
            for n in range(4 if start else 1):
                copy = pltpu.make_async_copy(sources[2 * n + p].at[pl.ds(base + first - r * geo.h1, end - first)], part, sem.at[3 + i])
                if start:
                    pl.when((own if n < 2 else ~own) & (kept if n % 2 == 0 else ~kept))(copy.start)
                else:
                    copy.wait()

    def copies(n, out):
        shape, matrix, at, *_, slot = units[n]
        *kept, _, sem, out_sem = rings[shape]
        wide = pl.ds(at * WIDE, WIDE)
        where = (0, slice(None), wide) if shape == TALL else (0, wide)
        for i in range(3):
            here, there = kept[i].at[slot], (results if out else given)[matrix + 7 * i].at[where]
            yield pltpu.make_async_copy(here, there, out_sem.at[slot, i]) if out else pltpu.make_async_copy(there, here, sem.at[slot, i])

    def enter(n, start):
        shape, _, _, geo, chunk, rows, slot = units[n]
        for copy in copies(n, 0):
            copy.start() if start else copy.wait()
        gradient(geo, chunk, rows, rings[shape][3].at[slot], rings[shape][4].at[slot], start)

    units, seen = [], {TALL: 0, FLAT: 0}
    for unit in _blocks(late):
        units.append((*unit, seen[unit[0]] % RING[unit[0]]))
        seen[unit[0]] += 1

    ready = 0
    busy = {}
    for n, (shape, *_, slot) in enumerate(units):
        while ready < len(units) and (ready <= n or ready - n < 5):
            key = units[ready][0], units[ready][-1]
            if key in busy:
                if busy[key] > n - 2 and ready > n:
                    break
                for copy in copies(busy.pop(key), 1):
                    copy.wait()
            enter(ready, 1)
            ready += 1
        enter(n, 0)
        w, m, v, g, *_ = rings[shape]

        def strip(i, _):
            size = 32 if shape == TALL else LANES
            rows = pl.ds(pl.multiple_of(i * size, size), size)
            grad = g[slot, rows, :].astype(F32) if shape == TALL else g[slot, :, rows].astype(F32).T
            new = adamw(w[slot, rows, :].astype(F32), m[slot, rows, :], v[slot, rows, :], grad * factor)
            w[slot, rows, :], m[slot, rows, :], v[slot, rows, :] = new

        lax.fori_loop(0, 24 if shape == TALL else 4, strip, None)
        for copy in copies(n, 1):
            copy.start()
        busy[shape, slot] = n
    for n in busy.values():
        for copy in copies(n, 1):
            copy.wait()


def update(squares, sources, arrays, done):
    anywhere, dma = pl.BlockSpec(memory_space=pl.ANY), pltpu.SemaphoreType.DMA
    scratch = []
    for shape, n in RING.items():
        scratch += [pltpu.VMEM((n, *shape), t) for t in (BF16, F32, F32)] + [pltpu.VMEM((n, *TALL), BF16), dma((n, 8)), dma((n, 3))]
    inputs = [*sources, *arrays, *done]
    size = sum(a.size for a in arrays)
    return pl.pallas_call(
        functools.partial(_update, late=len(sources) > 1),
        in_specs=[pl.BlockSpec(memory_space=pltpu.VMEM)] + [anywhere] * len(inputs),
        out_specs=[anywhere] * 21,
        out_shape=[jax.ShapeDtypeStruct(a.shape, a.dtype) for a in arrays],
        scratch_shapes=scratch,
        input_output_aliases={1 + len(inputs) - len(done) + i: i for i in range(len(done))},
        compiler_params=pltpu.CompilerParams(vmem_limit_bytes=VMEM),
        cost_estimate=pl.CostEstimate(flops=300 * size, transcendentals=0, bytes_accessed=4 * size),
    )(squares, *inputs)


def swaps():
    first, across = [[], []], [[], []]
    for d in range(256):
        core, y, x = d % 2, d // 16 % 4, d // 64
        for p, c, unit in ((0, x, 64), (1, y, 16)):
            peer = c + 1 - 2 * (c % 2) if core == p else 3 - c
            other = d + (peer - c) * unit
            first[p].append((d, other))
            across[p].append((d, other + 1 - 2 * core))
    return first, across, [(d, d + 1 - 2 * (d % 2)) for d in range(256)]


def rotary(tokens):
    half = HALF
    speed = THETA ** (-np.arange(half) / half)
    far, near = np.arange(0, tokens, 32)[:, None, None] * speed, np.arange(32)[:, None] * speed
    (ca, sa), (cb, sb) = ([f(a).astype(np.float32) for f in (np.cos, np.sin)] for a in (far, near))
    return (ca * jnp.asarray(cb) - sa * jnp.asarray(sb)).reshape(tokens, half), (sa * jnp.asarray(cb) + ca * jnp.asarray(sb)).reshape(tokens, half)


def solution(mesh):
    def step(x, dy, *arrays):
        wq, wk, wv, wo, wg, wu, wd = arrays[:7]
        cos, sin = rotary(x.shape[1])
        q, k, v, o, lse, at, h, b = attend(x[0], cos, sin, wq, wk, wv, wo)
        early, *late, squares = layer(b, dy[0], h, at, cos, sin, wg, wu, wd, q, k, v, o, lse, wo)
        first, across, cores = swaps()
        sources = [*late]
        for perms in (first, [cores] * 2, across):
            sources += [lax.ppermute(part, "dp", perm) for part, perm in zip(late, perms, strict=True)]
        done = update(squares, [early], arrays, [])
        return tuple(update(squares, sources, arrays, done))

    states, all_of = P(("rep", "dp")), P()
    return jax.shard_map(
        step,
        mesh=mesh,
        in_specs=(states, states) + (all_of,) * 21,
        out_specs=(P("rep"),) * 21,
        check_vma=False,
    )
```
